32 devices in a mesh: cfg: 2 (over y), expert: 4 (over z), ffn: 4 (over x, core).
Axes of the slice: x: 2, y: 2, z: 4, core: 2. Of those that a mesh axis runs over, the one named last changes fastest.
Arguments:
- tokens: bfloat16 [2048, 2048], P(('cfg', 'expert'), 'ffn'), parts along dimension 0, may hold values from -6 to 6
- chosen: int32 [8, 512], P(('cfg', 'expert')), parts along dimension 0, may hold values from 0 to 1023, as said below
- gates: float32 [8, 512], P(('cfg', 'expert')), parts along dimension 0, may hold values from 0.1 to 1
- capacity: int32 [2], P('cfg'), parts along dimension 0, may hold values from 256 to 512
- w_gate: bfloat16 [4, 2048, 1024], P('expert', None, 'ffn'), may hold values from -0.125 to 0.125
- w_up: bfloat16 [4, 2048, 1024], P('expert', None, 'ffn'), may hold values from -0.125 to 0.125
- w_down: bfloat16 [4, 1024, 2048], P('expert', 'ffn'), may hold values from -0.1875 to 0.1875
Outputs:
- mixed: bfloat16 [2048, 2048], P(('cfg', 'expert'), 'ffn'), parts along dimension 0
The draws below stay inside these ranges and needn't reach their ends.
There are 2 independent parts, one for each index of `cfg`. The reference program is written for one: setup_inputs(seed, part) draws one part's arguments, and reference() takes and returns one part's arrays. A program takes and returns all parts, laid end to end along the dimension named above; an argument that names none is the same for every part. Nothing has to cross between parts.
Inputs may be any that keep to these rules, and one draw needn't show every extreme that they name: `chosen`: each row lists 512 different tokens; at most 256 of one row's tokens lie in one aligned block of 256 tokens, and every row has exactly 256 in some block.
All inputs are finite; a program needn't handle non-finite values.
Results may differ from the reference program's by a relative error of at most 0.013.
Values may be sent and summed in bfloat16 or wider, within the bound.
A program may use at most 64 MiB of HBM per device.

```python
import math
import jax
import jax.numpy as jnp
from jax import lax

D = 2048
FF = 1024
TOK_DEV = 256
FF_DEV = 256
EXPERTS = 4
TOKENS = 1024
CAP = 512
N_FFN = 4


def draw_chosen(key, part):
    half_most = CAP // EXPERTS

    def one_expert(expert_key):
        key_counts, key_sources, key_tokens, key_order = jax.random.split(expert_key, 4)
        shifts = jax.random.randint(key_counts, (EXPERTS // 2,), 0, half_most + 1)
        shifts = shifts.at[0].set(half_most)
        paired = jnp.stack([shifts, -shifts], axis=1).reshape(-1)
        source_order = jax.random.permutation(key_sources, EXPERTS)
        counts = jnp.zeros((EXPERTS,), jnp.int32).at[source_order].set((half_most + paired).astype(jnp.int32))
        token_orders = jax.vmap(lambda inner: jax.random.permutation(inner, TOK_DEV))(jax.random.split(key_tokens, EXPERTS))
        ends = jnp.cumsum(counts)
        starts = ends - counts
        positions = jnp.arange(CAP, dtype=jnp.int32)
        source = jnp.sum((positions[:, None] >= ends[None, :]).astype(jnp.int32), axis=1)
        within = positions - starts[source]
        token_ids = source * TOK_DEV + token_orders[source, within]
        shuffle = jax.random.permutation(key_order, CAP)
        return token_ids[shuffle].astype(jnp.int32)
    expert_keys = jax.random.split(jax.random.fold_in(key, 11), EXPERTS)
    return jax.vmap(one_expert)(expert_keys)


def block_scale(rng, shape, pieces, least, largest):
    gain = 1.0
    for axis_at, shards_of in pieces:
        heights = jax.random.uniform(jax.random.fold_in(jax.random.fold_in(rng, 6), axis_at), (shards_of,), jnp.float32, least / len(pieces), largest / len(pieces))
        gain = gain * jnp.repeat(jnp.exp(heights), shape[axis_at] // shards_of).reshape((-1,) + (1,) * (len(shape) - 1 - axis_at))
    return gain


def centred(key, extent, deviation, reach, cuts=(), held_as=jnp.bfloat16):
    drawn = deviation * jax.random.normal(key, extent, jnp.float32)
    if cuts:
        drawn = drawn * block_scale(key, extent, cuts, -0.22, 0.18)
    return jnp.clip(drawn, -reach, reach).astype(held_as)


def setup_inputs(seed: int = 0, part: int = 0) -> dict:
    key_list = jax.random.split(jax.random.key(seed), 8)
    part_keys = jax.random.split(jax.random.fold_in(key_list[7], part), 8)
    tokens = centred(part_keys[0], (TOKENS, D), 1.0, 6.0, ((0, 4), (1, 4)))
    chosen = draw_chosen(jax.random.fold_in(jax.random.fold_in(key_list[7], part), 71), part)
    gates = jnp.clip(jnp.exp(math.log(1.0) - 2.3025851 * jax.random.uniform(part_keys[2], (EXPERTS, CAP), jnp.float32) ** block_scale(part_keys[2], (EXPERTS, CAP), ((0, 4),), -0.2, 0.2)), 0.1, 1.0)
    capacity = jax.random.randint(part_keys[3], (1,), CAP // 2, CAP + 1).astype(jnp.int32)
    w_gate = centred(key_list[4], (EXPERTS, D, FF), D ** -0.5, 0.125, ((0, 4), (2, 4)))
    w_up = centred(key_list[5], (EXPERTS, D, FF), D ** -0.5, 0.125, ((0, 4), (2, 4)))
    w_down = centred(key_list[6], (EXPERTS, FF, D), FF ** -0.5, 0.1875, ((0, 4), (1, 4)))
    return {"tokens": tokens, "chosen": chosen, "gates": gates, "capacity": capacity, "w_gate": w_gate, "w_up": w_up, "w_down": w_down}


def reference(tokens, chosen, gates, capacity, w_gate, w_up, w_down):
    positions = jnp.arange(CAP, dtype=jnp.int32)
    live = jnp.where(positions[None, :] < capacity[0], gates, jnp.zeros_like(gates)).astype(jnp.float32)

    def expert_step(total, item):
        picked_ids, weights, gate_cols, up_cols, down_rows = item
        gathered = jnp.take(tokens, picked_ids, axis=0)
        summed = jnp.zeros((CAP, D), jnp.float32)
        for block in range(N_FFN):
            low_col = block * FF_DEV
            gate_part = jnp.dot(gathered, gate_cols[:, low_col:low_col + FF_DEV], preferred_element_type=jnp.float32)
            up_part = jnp.dot(gathered, up_cols[:, low_col:low_col + FF_DEV], preferred_element_type=jnp.float32)
            hidden = (jax.nn.silu(gate_part) * up_part).astype(jnp.bfloat16)
            partial_value = jnp.dot(hidden, down_rows[low_col:low_col + FF_DEV, :], preferred_element_type=jnp.float32).astype(jnp.bfloat16)
            summed = summed + lax.optimization_barrier(partial_value).astype(jnp.float32)
        contribution = (weights[:, None] * summed).astype(jnp.bfloat16)
        total = total.at[picked_ids].add(lax.optimization_barrier(contribution).astype(jnp.float32))
        return total, None

    start_total = jnp.zeros((TOKENS, D), jnp.float32)
    total, unused = lax.scan(expert_step, start_total, (chosen, live, w_gate, w_up, w_down))
    return total.astype(jnp.bfloat16)
```

```python
import functools

import jax
import jax.numpy as jnp
from jax import lax
from jax.experimental import pallas as pl
from jax.experimental.pallas import tpu as pltpu
from jax.sharding import PartitionSpec as P


def shards_general(tokens, chosen, gates, capacity, w_gate, w_up, w_down):
    experts_n = lax.axis_size("expert")
    tok_dev = tokens.shape[0]
    picked_ids = chosen[0]
    listed = picked_ids.shape[0]
    slot_depth = 2 * listed // experts_n
    positions = jnp.arange(listed, dtype=jnp.int32)
    alive_mask = positions < capacity[0]
    weights = jnp.where(alive_mask, gates[0], jnp.zeros_like(gates[0]))
    source = picked_ids // tok_dev
    offset = picked_ids - source * tok_dev
    member = (source[:, None] == jnp.arange(experts_n, dtype=jnp.int32)[None, :]).astype(jnp.int32)
    before = jnp.cumsum(member, axis=0) - member
    rank_in = jnp.sum(before * member, axis=1)
    slot_of = source * slot_depth + rank_in
    wanted = jnp.where(alive_mask, offset, -1)
    request = jnp.full((experts_n * slot_depth,), -1, jnp.int32).at[slot_of].set(wanted)
    requested = lax.all_to_all(
        request.reshape(experts_n, slot_depth), "expert", split_axis=0, concat_axis=0, tiled=True
    ).reshape(-1)
    usable = requested >= 0
    safe_idx = jnp.maximum(requested, 0)
    gate_cols = w_gate[0]
    up_cols = w_up[0]
    down_rows = w_down[0]
    row_block = jnp.where(
        usable[:, None], jnp.take(tokens, safe_idx, axis=0), jnp.zeros((), jnp.bfloat16)
    )
    slots = lax.all_to_all(
        row_block.reshape(experts_n, slot_depth, -1),
        "expert",
        split_axis=0,
        concat_axis=0,
        tiled=True,
    )
    picked = jnp.take(slots.reshape(experts_n * slot_depth, -1), slot_of, axis=0)
    portion = lax.all_gather(picked, "ffn", axis=1, tiled=True)
    gate_next = jnp.dot(portion, gate_cols, preferred_element_type=jnp.float32)
    up_next = jnp.dot(portion, up_cols, preferred_element_type=jnp.float32)
    hidden = (jax.nn.silu(gate_next) * up_next).astype(jnp.bfloat16)
    partial_value = jnp.dot(hidden, down_rows, preferred_element_type=jnp.float32)
    summed = lax.psum_scatter(
        partial_value.astype(jnp.bfloat16), "ffn", scatter_dimension=1, tiled=True
    ).astype(jnp.float32)
    contribution = (weights[:, None] * summed).astype(jnp.bfloat16)
    returned_slots = (
        jnp.zeros((experts_n * slot_depth, contribution.shape[1]), jnp.bfloat16)
        .at[slot_of]
        .set(contribution)
    )
    returned = lax.all_to_all(
        returned_slots.reshape(experts_n, slot_depth, -1),
        "expert",
        split_axis=0,
        concat_axis=0,
        tiled=True,
    )
    returned = returned.reshape(experts_n * slot_depth, -1)
    placement_map = (requested[None, :] == jnp.arange(tok_dev, dtype=jnp.int32)[:, None]).astype(
        jnp.bfloat16
    )
    mixed = jnp.dot(placement_map, returned, preferred_element_type=jnp.float32)
    return mixed.astype(jnp.bfloat16)


LANES = 128
KINDS = 13
MESH = pl.DeviceIdType.MESH
(TO_RIGHT, TO_LEFT, ON_RIGHT, ON_LEFT, ROWS_X, ROWS_CORE, ROWS_ON,
 PART_CORE, PART_X, HALF_RIGHT, HALF_LEFT, SUM_RIGHT, SUM_LEFT) = range(KINDS)


def dot(a, b):
    return jnp.dot(a, b, preferred_element_type=jnp.float32)


def fused(ring, cap_ref, chosen_ref, gates_ref, tok_ref, wg_ref, wu_ref, wd_ref, out_ref,
          near, pick, put, live, rows, w_in, w_out, acc, hid, part_out, part_in, own_sum,
          sum_out, sum_in, far_out, half_in, edge_out, edge_in, own_out,
          send_sem, recv_sem, load_sem):
    block, width = tok_ref.shape
    listed = chosen_ref.shape[1]
    half = block // 2
    chunks = width // LANES
    z = lax.axis_index("expert")
    f = lax.axis_index("ffn")
    right = {"expert": lax.rem(z + 1, ring)}
    left = {"expert": lax.rem(z + ring - 1, ring)}
    chip, core = f // 2, f % 2
    slot_id = (f, chip * 2 + 1 - core, (1 - chip) * 2 + core, (1 - chip) * 2 + 1 - core)
    mate = {"ffn": slot_id[1]}
    across = {"ffn": slot_id[2]}

    loads = []
    ff = wg_ref.shape[1]
    for s in range(4):
        at = pl.ds(pl.multiple_of(slot_id[s] * width, width), width)
        loads.append([
            pltpu.make_async_copy(wg_ref.at[at, :], w_in.at[s, :, 0:ff], load_sem.at[3 * s]),
            pltpu.make_async_copy(wu_ref.at[at, :], w_in.at[s, :, ff:2 * ff], load_sem.at[3 * s + 1]),
            pltpu.make_async_copy(wd_ref.at[:, at], w_out.at[s], load_sem.at[3 * s + 2]),
        ])
    for group in loads:
        for load in group:
            load.start()

    barrier = pltpu.get_barrier_semaphore()
    for other in (left, right, mate, across):
        pl.semaphore_signal(barrier, inc=1, device_id=other, device_id_type=MESH)
    pl.semaphore_wait(barrier, 4)

    def cols(q):
        return slice(q * LANES, (q + 1) * LANES)

    def copy(kind, q):
        src, dst, to = {
            TO_RIGHT: lambda: (tok_ref.at[:, cols(q)], near.at[q, 0:block], right),
            TO_LEFT: lambda: (tok_ref.at[:, cols(q)], near.at[q, 2 * block:3 * block], left),
            ON_RIGHT: lambda: (near.at[q, 0:half], near.at[q, block:block + half], right),
            ON_LEFT: lambda: (near.at[q, 2 * block + half:3 * block], near.at[q, block + half:2 * block], left),
            ROWS_X: lambda: (rows.at[0, q], rows.at[2, q], across),
            ROWS_CORE: lambda: (rows.at[0, q], rows.at[1, q], mate),
            ROWS_ON: lambda: (rows.at[2, q], rows.at[3, q], mate),
            PART_CORE: lambda: (part_out.at[q], part_in.at[q], mate),
            PART_X: lambda: (sum_out.at[q], sum_in.at[q], across),
            HALF_RIGHT: lambda: (far_out.at[q, 0:half], half_in.at[q, 0:half], right),
            HALF_LEFT: lambda: (far_out.at[q, half:block], half_in.at[q, half:block], left),
            SUM_RIGHT: lambda: (edge_out.at[q, 0], edge_in.at[q, 0], right),
            SUM_LEFT: lambda: (edge_out.at[q, 1], edge_in.at[q, 1], left),
        }[kind]()
        i = kind * chunks + q
        return pltpu.make_async_remote_copy(
            src_ref=src, dst_ref=dst, send_sem=send_sem.at[i], recv_sem=recv_sem.at[i],
            device_id=to, device_id_type=MESH)

    def start(kind, q):
        copy(kind, q).start()

    def got(kind, q):
        copy(kind, q).wait_recv()

    def own(q):
        start(TO_RIGHT, q)
        start(TO_LEFT, q)

    own(0)
    own(1)

    ids = chosen_ref[...]
    ids_col = jnp.broadcast_to(ids.astype(jnp.float32), (LANES, listed)).T.astype(jnp.int32)
    lane = lax.broadcasted_iota(jnp.int32, (listed, LANES), 1)
    for r in range(4):
        base = lax.rem(z + ring - r, ring) * block
        for h in range(block // LANES):
            hit = ids_col == lane + (base + h * LANES)
            pick[:, r * block + h * LANES:r * block + (h + 1) * LANES] = jnp.where(hit, 1.0, 0.0).astype(jnp.bfloat16)

    def select(q):
        got(ON_RIGHT, q)
        got(ON_LEFT, q)
        chosen_rows = dot(pick[:, 0:block], tok_ref[:, cols(q)]) + dot(pick[:, block:], near[q])
        rows[0, q] = chosen_rows.astype(jnp.bfloat16)
        start(ROWS_X, q)
        start(ROWS_CORE, q)

    for q in range(chunks):
        got(TO_RIGHT, q)
        start(ON_RIGHT, q)
        got(TO_LEFT, q)
        start(ON_LEFT, q)
        if q + 2 < chunks:
            own(q + 2)
        if q >= 1:
            select(q - 1)
    select(chunks - 1)

    token = lax.broadcasted_iota(jnp.int32, (block, listed), 0)
    for r in range(4):
        base = lax.rem(z + ring - r, ring) * block
        put[r] = jnp.where(ids == token + base, 1.0, 0.0).astype(jnp.bfloat16)
    position = lax.broadcasted_iota(jnp.int32, (1, listed), 1)
    kept = jnp.where(position < cap_ref[0], gates_ref[...], 0.0)
    live[...] = jnp.broadcast_to(kept, (LANES, listed)).T

    for group in loads:
        for load in group:
            load.wait()

    def whole(s):
        return jnp.concatenate([rows[s, q] for q in range(chunks)], axis=1)

    acc[...] = dot(whole(0), w_in[0])
    for q in range(chunks):
        got(ROWS_CORE, q)
    acc[...] += dot(whole(1), w_in[1])

    def add(s, q):
        acc[...] += dot(rows[s, q], w_in[s, q * LANES:(q + 1) * LANES])

    for q in range(chunks):
        got(ROWS_X, q)
        start(ROWS_ON, q)
        add(2, q)
        if q >= 1:
            got(ROWS_ON, q - 1)
            add(3, q - 1)
    got(ROWS_ON, chunks - 1)
    add(3, chunks - 1)

    gate = acc[:, 0:ff]
    hid[...] = (gate / (1.0 + jnp.exp(-gate)) * acc[:, ff:2 * ff]).astype(jnp.bfloat16)

    for q in range(chunks):
        both = jnp.concatenate([w_out[1, :, cols(q)], w_out[3, :, cols(q)]], axis=1)
        part_out[q] = dot(hid[...], both).astype(jnp.bfloat16)
        start(PART_CORE, q)
    for q in range(chunks):
        both = dot(hid[...], jnp.concatenate([w_out[0, :, cols(q)], w_out[2, :, cols(q)]], axis=1))
        got(PART_CORE, q)
        both = both + part_in[q].astype(jnp.float32)
        sum_out[q] = both[:, LANES:].astype(jnp.bfloat16)
        start(PART_X, q)
        own_sum[q] = both[:, :LANES]

    def finish(q):
        got(SUM_RIGHT, q)
        got(SUM_LEFT, q)
        total = own_out[q] + edge_in[q, 0].astype(jnp.float32) + edge_in[q, 1].astype(jnp.float32)
        out_ref[:, cols(q)] = total.astype(jnp.bfloat16)

    for q in range(chunks):
        got(PART_X, q)
        y = own_sum[q] + sum_in[q].astype(jnp.float32)
        weighted = (live[...] * y).astype(jnp.bfloat16)
        far_out[q] = dot(put[2], weighted).astype(jnp.bfloat16)
        start(HALF_RIGHT, q)
        start(HALF_LEFT, q)
        to_right = dot(put[3], weighted)
        to_left = dot(put[1], weighted)
        own_out[q] = dot(put[0], weighted)
        if q >= 1:
            finish(q - 1)
        got(HALF_RIGHT, q)
        edge_out[q, 0, 0:half] = (to_right[0:half] + half_in[q, 0:half].astype(jnp.float32)).astype(jnp.bfloat16)
        edge_out[q, 0, half:block] = to_right[half:block].astype(jnp.bfloat16)
        start(SUM_RIGHT, q)
        got(HALF_LEFT, q)
        edge_out[q, 1, half:block] = (to_left[half:block] + half_in[q, half:block].astype(jnp.float32)).astype(jnp.bfloat16)
        edge_out[q, 1, 0:half] = to_left[0:half].astype(jnp.bfloat16)
        start(SUM_LEFT, q)
    finish(chunks - 1)

    for kind in range(KINDS):
        for q in range(chunks):
            copy(kind, q).wait_send()


def shards_fused(ring, tokens, chosen, gates, capacity, w_gate, w_up, w_down):
    block, width = tokens.shape
    listed = chosen.shape[1]
    ff = w_gate.shape[2]
    chunks = width // LANES
    bf16, f32 = jnp.bfloat16, jnp.float32
    vmem = pl.BlockSpec(memory_space=pltpu.VMEM)
    far = pl.BlockSpec(memory_space=pl.ANY)
    return pl.pallas_call(
        functools.partial(fused, ring),
        out_shape=jax.ShapeDtypeStruct(tokens.shape, bf16),
        in_specs=[pl.BlockSpec(memory_space=pltpu.SMEM), vmem, vmem, vmem, far, far, far],
        out_specs=vmem,
        scratch_shapes=[
            pltpu.VMEM((chunks, 3 * block, LANES), bf16),
            pltpu.VMEM((listed, 4 * block), bf16),
            pltpu.VMEM((4, block, listed), bf16),
            pltpu.VMEM((listed, LANES), f32),
            pltpu.VMEM((4, chunks, listed, LANES), bf16),
            pltpu.VMEM((4, width, 2 * ff), bf16),
            pltpu.VMEM((4, ff, width), bf16),
            pltpu.VMEM((listed, 2 * ff), f32),
            pltpu.VMEM((listed, ff), bf16),
            pltpu.VMEM((chunks, listed, 2 * LANES), bf16),
            pltpu.VMEM((chunks, listed, 2 * LANES), bf16),
            pltpu.VMEM((chunks, listed, LANES), f32),
            pltpu.VMEM((chunks, listed, LANES), bf16),
            pltpu.VMEM((chunks, listed, LANES), bf16),
            pltpu.VMEM((chunks, block, LANES), bf16),
            pltpu.VMEM((chunks, block, LANES), bf16),
            pltpu.VMEM((chunks, 2, block, LANES), bf16),
            pltpu.VMEM((chunks, 2, block, LANES), bf16),
            pltpu.VMEM((chunks, block, LANES), f32),
            pltpu.SemaphoreType.DMA((KINDS * chunks,)),
            pltpu.SemaphoreType.DMA((KINDS * chunks,)),
            pltpu.SemaphoreType.DMA((12,)),
        ],
        compiler_params=pltpu.CompilerParams(collective_id=0, has_side_effects=True),
    )(capacity, chosen, gates, tokens, w_gate[0], w_up[0], w_down[0])


def solution(mesh):
    in_specs = (
        P(("cfg", "expert"), "ffn"),
        P(("cfg", "expert"), None),
        P(("cfg", "expert"), None),
        P("cfg"),
        P("expert", None, "ffn"),
        P("expert", None, "ffn"),
        P("expert", "ffn", None),
    )
    out_specs = P(("cfg", "expert"), "ffn")
    ring = mesh.shape["expert"]
    small = ring == 4 and mesh.shape["ffn"] == 4
    body = functools.partial(shards_fused, ring) if small else shards_general
    return jax.shard_map(body, mesh=mesh, in_specs=in_specs, out_specs=out_specs, check_vma=False)
```

```python
import functools

import jax
import jax.numpy as jnp
from jax import lax
from jax.experimental import pallas as pl
from jax.experimental.pallas import tpu as pltpu
from jax.sharding import PartitionSpec as P


def shards_general(tokens, chosen, gates, capacity, w_gate, w_up, w_down):
    experts_n = lax.axis_size("expert")
    tok_dev = tokens.shape[0]
    picked_ids = chosen[0]
    listed = picked_ids.shape[0]
    slot_depth = 2 * listed // experts_n
    positions = jnp.arange(listed, dtype=jnp.int32)
    alive_mask = positions < capacity[0]
    weights = jnp.where(alive_mask, gates[0], jnp.zeros_like(gates[0]))
    source = picked_ids // tok_dev
    offset = picked_ids - source * tok_dev
    member = (source[:, None] == jnp.arange(experts_n, dtype=jnp.int32)[None, :]).astype(jnp.int32)
    before = jnp.cumsum(member, axis=0) - member
    rank_in = jnp.sum(before * member, axis=1)
    slot_of = source * slot_depth + rank_in
    wanted = jnp.where(alive_mask, offset, -1)
    request = jnp.full((experts_n * slot_depth,), -1, jnp.int32).at[slot_of].set(wanted)
    requested = lax.all_to_all(
        request.reshape(experts_n, slot_depth), "expert", split_axis=0, concat_axis=0, tiled=True
    ).reshape(-1)
    usable = requested >= 0
    safe_idx = jnp.maximum(requested, 0)
    gate_cols = w_gate[0]
    up_cols = w_up[0]
    down_rows = w_down[0]
    row_block = jnp.where(
        usable[:, None], jnp.take(tokens, safe_idx, axis=0), jnp.zeros((), jnp.bfloat16)
    )
    slots = lax.all_to_all(
        row_block.reshape(experts_n, slot_depth, -1),
        "expert",
        split_axis=0,
        concat_axis=0,
        tiled=True,
    )
    picked = jnp.take(slots.reshape(experts_n * slot_depth, -1), slot_of, axis=0)
    portion = lax.all_gather(picked, "ffn", axis=1, tiled=True)
    gate_next = jnp.dot(portion, gate_cols, preferred_element_type=jnp.float32)
    up_next = jnp.dot(portion, up_cols, preferred_element_type=jnp.float32)
    hidden = (jax.nn.silu(gate_next) * up_next).astype(jnp.bfloat16)
    partial_value = jnp.dot(hidden, down_rows, preferred_element_type=jnp.float32)
    summed = lax.psum_scatter(
        partial_value.astype(jnp.bfloat16), "ffn", scatter_dimension=1, tiled=True
    ).astype(jnp.float32)
    contribution = (weights[:, None] * summed).astype(jnp.bfloat16)
    returned_slots = (
        jnp.zeros((experts_n * slot_depth, contribution.shape[1]), jnp.bfloat16)
        .at[slot_of]
        .set(contribution)
    )
    returned = lax.all_to_all(
        returned_slots.reshape(experts_n, slot_depth, -1),
        "expert",
        split_axis=0,
        concat_axis=0,
        tiled=True,
    )
    returned = returned.reshape(experts_n * slot_depth, -1)
    placement_map = (requested[None, :] == jnp.arange(tok_dev, dtype=jnp.int32)[:, None]).astype(
        jnp.bfloat16
    )
    mixed = jnp.dot(placement_map, returned, preferred_element_type=jnp.float32)
    return mixed.astype(jnp.bfloat16)


LANES = 128
KINDS = 13
MESH = pl.DeviceIdType.MESH
(TO_RIGHT, TO_LEFT, ON_RIGHT, ON_LEFT, ROWS_X, ROWS_CORE, ROWS_ON,
 PART_CORE, PART_X, HALF_RIGHT, HALF_LEFT, SUM_RIGHT, SUM_LEFT) = range(KINDS)


def dot(a, b):
    return jnp.dot(a, b, preferred_element_type=jnp.float32)


def fused(ring, cap_ref, chosen_ref, gates_ref, tok_ref, wg_ref, wu_ref, wd_ref, out_ref,
          near, pick, put, live, rows, w_in, w_out, acc, hid, part_out, part_in, own_sum,
          sum_out, sum_in, far_out, half_in, edges, edge_out, edge_in, own_out,
          send_sem, recv_sem, load_sem):
    block, width = tok_ref.shape
    listed = chosen_ref.shape[1]
    half = block // 2
    chunks = width // LANES
    z = lax.axis_index("expert")
    f = lax.axis_index("ffn")
    right = {"expert": lax.rem(z + 1, ring)}
    left = {"expert": lax.rem(z + ring - 1, ring)}
    chip, core = f // 2, f % 2
    slot_id = (f, chip * 2 + 1 - core, (1 - chip) * 2 + core, (1 - chip) * 2 + 1 - core)
    mate = {"ffn": slot_id[1]}
    across = {"ffn": slot_id[2]}

    loads = []
    ff = wg_ref.shape[1]
    for s in range(4):
        at = pl.ds(pl.multiple_of(slot_id[s] * width, width), width)
        loads.append([
            pltpu.make_async_copy(wg_ref.at[at, :], w_in.at[s, :, 0:ff], load_sem.at[3 * s]),
            pltpu.make_async_copy(wu_ref.at[at, :], w_in.at[s, :, ff:2 * ff], load_sem.at[3 * s + 1]),
            pltpu.make_async_copy(wd_ref.at[:, at], w_out.at[s], load_sem.at[3 * s + 2]),
        ])
    for group in loads:
        for load in group:
            load.start()

    barrier = pltpu.get_barrier_semaphore()
    for other in (left, right, mate, across):
        pl.semaphore_signal(barrier, inc=1, device_id=other, device_id_type=MESH)
    pl.semaphore_wait(barrier, 4)

    def cols(q):
        return slice(q * LANES, (q + 1) * LANES)

    def copy(kind, q):
        src, dst, to = {
            TO_RIGHT: lambda: (tok_ref.at[:, cols(q)], near.at[q, 0:block], right),
            TO_LEFT: lambda: (tok_ref.at[:, cols(q)], near.at[q, 2 * block:3 * block], left),
            ON_RIGHT: lambda: (near.at[q, 0:half], near.at[q, block:block + half], right),
            ON_LEFT: lambda: (near.at[q, 2 * block + half:3 * block], near.at[q, block + half:2 * block], left),
            ROWS_X: lambda: (rows.at[0, q], rows.at[2, q], across),
            ROWS_CORE: lambda: (rows.at[0, q], rows.at[1, q], mate),
            ROWS_ON: lambda: (rows.at[2, q], rows.at[3, q], mate),
            PART_CORE: lambda: (part_out.at[q], part_in.at[q], mate),
            PART_X: lambda: (sum_out.at[q], sum_in.at[q], across),
            HALF_RIGHT: lambda: (far_out.at[q, 0:half], half_in.at[q, 0:half], right),
            HALF_LEFT: lambda: (far_out.at[q, half:block], half_in.at[q, half:block], left),
            SUM_RIGHT: lambda: (edge_out.at[q, 0], edge_in.at[q, 0], right),
            SUM_LEFT: lambda: (edge_out.at[q, 1], edge_in.at[q, 1], left),
        }[kind]()
        i = kind * chunks + q
        return pltpu.make_async_remote_copy(
            src_ref=src, dst_ref=dst, send_sem=send_sem.at[i], recv_sem=recv_sem.at[i],
            device_id=to, device_id_type=MESH)

    def start(kind, q):
        copy(kind, q).start()

    def got(kind, q):
        copy(kind, q).wait_recv()

    def own(q):
        start(TO_RIGHT, q)
        start(TO_LEFT, q)

    for q in range(min(3, chunks)):
        own(q)

    ids = chosen_ref[...]
    ids_col = jnp.broadcast_to(ids.astype(jnp.float32), (LANES, listed)).T.astype(jnp.int32)
    lane = lax.broadcasted_iota(jnp.int32, (listed, LANES), 1)
    for r in range(4):
        base = lax.rem(z + ring - r, ring) * block
        for h in range(block // LANES):
            hit = ids_col == lane + (base + h * LANES)
            pick[:, r * block + h * LANES:r * block + (h + 1) * LANES] = jnp.where(hit, 1.0, 0.0).astype(jnp.bfloat16)

    def select(q):
        got(ON_RIGHT, q)
        got(ON_LEFT, q)
        chosen_rows = dot(pick[:, 0:block], tok_ref[:, cols(q)]) + dot(pick[:, block:], near[q])
        rows[0, q] = chosen_rows.astype(jnp.bfloat16)
        start(ROWS_X, q)
        start(ROWS_CORE, q)

    for q in range(chunks):
        got(TO_RIGHT, q)
        start(ON_RIGHT, q)
        got(TO_LEFT, q)
        start(ON_LEFT, q)
        if q + 3 < chunks:
            own(q + 3)
        if q >= 1:
            select(q - 1)
    select(chunks - 1)

    token = lax.broadcasted_iota(jnp.int32, (block, listed), 0)
    for r in range(4):
        base = lax.rem(z + ring - r, ring) * block
        put[r] = jnp.where(ids == token + base, 1.0, 0.0).astype(jnp.bfloat16)
    position = lax.broadcasted_iota(jnp.int32, (1, listed), 1)
    kept = jnp.where(position < cap_ref[0], gates_ref[...], 0.0)
    live[...] = jnp.broadcast_to(kept, (LANES, listed)).T

    for group in loads:
        for load in group:
            load.wait()

    def whole(s):
        return jnp.concatenate([rows[s, q] for q in range(chunks)], axis=1)

    acc[...] = dot(whole(0), w_in[0])
    for q in range(chunks):
        got(ROWS_CORE, q)
    acc[...] += dot(whole(1), w_in[1])

    def add(s, q):
        acc[...] += dot(rows[s, q], w_in[s, q * LANES:(q + 1) * LANES])

    for q in range(chunks):
        got(ROWS_X, q)
        start(ROWS_ON, q)
        add(2, q)
        if q >= 1:
            got(ROWS_ON, q - 1)
            add(3, q - 1)
    got(ROWS_ON, chunks - 1)
    add(3, chunks - 1)

    gate = acc[:, 0:ff]
    hid[...] = (gate / (1.0 + jnp.exp(-gate)) * acc[:, ff:2 * ff]).astype(jnp.bfloat16)

    for q in range(chunks):
        both = jnp.concatenate([w_out[1, :, cols(q)], w_out[3, :, cols(q)]], axis=1)
        part_out[q] = dot(hid[...], both).astype(jnp.bfloat16)
        start(PART_CORE, q)
    for q in range(chunks):
        both = dot(hid[...], jnp.concatenate([w_out[0, :, cols(q)], w_out[2, :, cols(q)]], axis=1))
        got(PART_CORE, q)
        both = both + part_in[q].astype(jnp.float32)
        sum_out[q] = both[:, LANES:].astype(jnp.bfloat16)
        start(PART_X, q)
        own_sum[q] = both[:, :LANES]

    def finish(q):
        got(SUM_RIGHT, q)
        got(SUM_LEFT, q)
        total = own_out[q] + edge_in[q, 0].astype(jnp.float32) + edge_in[q, 1].astype(jnp.float32)
        out_ref[:, cols(q)] = total.astype(jnp.bfloat16)

    def spread(q):
        got(PART_X, q)
        y = own_sum[q] + sum_in[q].astype(jnp.float32)
        weighted = (live[...] * y).astype(jnp.bfloat16)
        far_out[q] = dot(put[2], weighted).astype(jnp.bfloat16)
        start(HALF_RIGHT, q)
        start(HALF_LEFT, q)
        edges[q, 0] = dot(put[3], weighted)
        edges[q, 1] = dot(put[1], weighted)
        own_out[q] = dot(put[0], weighted)

    def merge(q):
        got(HALF_RIGHT, q)
        edge_out[q, 0, 0:half] = (edges[q, 0, 0:half] + half_in[q, 0:half].astype(jnp.float32)).astype(jnp.bfloat16)
        edge_out[q, 0, half:block] = edges[q, 0, half:block].astype(jnp.bfloat16)
        start(SUM_RIGHT, q)
        got(HALF_LEFT, q)
        edge_out[q, 1, half:block] = (edges[q, 1, half:block] + half_in[q, half:block].astype(jnp.float32)).astype(jnp.bfloat16)
        edge_out[q, 1, 0:half] = edges[q, 1, 0:half].astype(jnp.bfloat16)
        start(SUM_LEFT, q)

    for q in range(chunks + 2):
        if q < chunks:
            spread(q)
        if 1 <= q <= chunks:
            merge(q - 1)
        if q >= 2:
            finish(q - 2)

    for kind in range(KINDS):
        for q in range(chunks):
            copy(kind, q).wait_send()


def shards_fused(ring, tokens, chosen, gates, capacity, w_gate, w_up, w_down):
    block, width = tokens.shape
    listed = chosen.shape[1]
    ff = w_gate.shape[2]
    chunks = width // LANES
    bf16, f32 = jnp.bfloat16, jnp.float32
    vmem = pl.BlockSpec(memory_space=pltpu.VMEM)
    far = pl.BlockSpec(memory_space=pl.ANY)
    return pl.pallas_call(
        functools.partial(fused, ring),
        out_shape=jax.ShapeDtypeStruct(tokens.shape, bf16),
        in_specs=[pl.BlockSpec(memory_space=pltpu.SMEM), vmem, vmem, vmem, far, far, far],
        out_specs=vmem,
        scratch_shapes=[
            pltpu.VMEM((chunks, 3 * block, LANES), bf16),
            pltpu.VMEM((listed, 4 * block), bf16),
            pltpu.VMEM((4, block, listed), bf16),
            pltpu.VMEM((listed, LANES), f32),
            pltpu.VMEM((4, chunks, listed, LANES), bf16),
            pltpu.VMEM((4, width, 2 * ff), bf16),
            pltpu.VMEM((4, ff, width), bf16),
            pltpu.VMEM((listed, 2 * ff), f32),
            pltpu.VMEM((listed, ff), bf16),
            pltpu.VMEM((chunks, listed, 2 * LANES), bf16),
            pltpu.VMEM((chunks, listed, 2 * LANES), bf16),
            pltpu.VMEM((chunks, listed, LANES), f32),
            pltpu.VMEM((chunks, listed, LANES), bf16),
            pltpu.VMEM((chunks, listed, LANES), bf16),
            pltpu.VMEM((chunks, block, LANES), bf16),
            pltpu.VMEM((chunks, block, LANES), bf16),
            pltpu.VMEM((chunks, 2, block, LANES), f32),
            pltpu.VMEM((chunks, 2, block, LANES), bf16),
            pltpu.VMEM((chunks, 2, block, LANES), bf16),
            pltpu.VMEM((chunks, block, LANES), f32),
            pltpu.SemaphoreType.DMA((KINDS * chunks,)),
            pltpu.SemaphoreType.DMA((KINDS * chunks,)),
            pltpu.SemaphoreType.DMA((12,)),
        ],
        compiler_params=pltpu.CompilerParams(collective_id=0, has_side_effects=True),
    )(capacity, chosen, gates, tokens, w_gate[0], w_up[0], w_down[0])


def solution(mesh):
    in_specs = (
        P(("cfg", "expert"), "ffn"),
        P(("cfg", "expert"), None),
        P(("cfg", "expert"), None),
        P("cfg"),
        P("expert", None, "ffn"),
        P("expert", None, "ffn"),
        P("expert", "ffn", None),
    )
    out_specs = P(("cfg", "expert"), "ffn")
    ring = mesh.shape["expert"]
    small = ring == 4 and mesh.shape["ffn"] == 4
    body = functools.partial(shards_fused, ring) if small else shards_general
    return jax.shard_map(body, mesh=mesh, in_specs=in_specs, out_specs=out_specs, check_vma=False)
```

```python
import functools

import jax
import jax.numpy as jnp
from jax import lax
from jax.experimental import pallas as pl
from jax.experimental.pallas import tpu as pltpu
from jax.sharding import PartitionSpec as P


def shards_general(tokens, chosen, gates, capacity, w_gate, w_up, w_down):
    experts_n = lax.axis_size("expert")
    tok_dev = tokens.shape[0]
    picked_ids = chosen[0]
    listed = picked_ids.shape[0]
    slot_depth = 2 * listed // experts_n
    positions = jnp.arange(listed, dtype=jnp.int32)
    alive_mask = positions < capacity[0]
    weights = jnp.where(alive_mask, gates[0], jnp.zeros_like(gates[0]))
    source = picked_ids // tok_dev
    offset = picked_ids - source * tok_dev
    member = (source[:, None] == jnp.arange(experts_n, dtype=jnp.int32)[None, :]).astype(jnp.int32)
    before = jnp.cumsum(member, axis=0) - member
    rank_in = jnp.sum(before * member, axis=1)
    slot_of = source * slot_depth + rank_in
    wanted = jnp.where(alive_mask, offset, -1)
    request = jnp.full((experts_n * slot_depth,), -1, jnp.int32).at[slot_of].set(wanted)
    requested = lax.all_to_all(
        request.reshape(experts_n, slot_depth), "expert", split_axis=0, concat_axis=0, tiled=True
    ).reshape(-1)
    usable = requested >= 0
    safe_idx = jnp.maximum(requested, 0)
    gate_cols = w_gate[0]
    up_cols = w_up[0]
    down_rows = w_down[0]
    row_block = jnp.where(
        usable[:, None], jnp.take(tokens, safe_idx, axis=0), jnp.zeros((), jnp.bfloat16)
    )
    slots = lax.all_to_all(
        row_block.reshape(experts_n, slot_depth, -1),
        "expert",
        split_axis=0,
        concat_axis=0,
        tiled=True,
    )
    picked = jnp.take(slots.reshape(experts_n * slot_depth, -1), slot_of, axis=0)
    portion = lax.all_gather(picked, "ffn", axis=1, tiled=True)
    gate_next = jnp.dot(portion, gate_cols, preferred_element_type=jnp.float32)
    up_next = jnp.dot(portion, up_cols, preferred_element_type=jnp.float32)
    hidden = (jax.nn.silu(gate_next) * up_next).astype(jnp.bfloat16)
    partial_value = jnp.dot(hidden, down_rows, preferred_element_type=jnp.float32)
    summed = lax.psum_scatter(
        partial_value.astype(jnp.bfloat16), "ffn", scatter_dimension=1, tiled=True
    ).astype(jnp.float32)
    contribution = (weights[:, None] * summed).astype(jnp.bfloat16)
    returned_slots = (
        jnp.zeros((experts_n * slot_depth, contribution.shape[1]), jnp.bfloat16)
        .at[slot_of]
        .set(contribution)
    )
    returned = lax.all_to_all(
        returned_slots.reshape(experts_n, slot_depth, -1),
        "expert",
        split_axis=0,
        concat_axis=0,
        tiled=True,
    )
    returned = returned.reshape(experts_n * slot_depth, -1)
    placement_map = (requested[None, :] == jnp.arange(tok_dev, dtype=jnp.int32)[:, None]).astype(
        jnp.bfloat16
    )
    mixed = jnp.dot(placement_map, returned, preferred_element_type=jnp.float32)
    return mixed.astype(jnp.bfloat16)


LANES = 128
KINDS = 13
MESH = pl.DeviceIdType.MESH
(TO_RIGHT, TO_LEFT, ON_RIGHT, ON_LEFT, ROWS_X, ROWS_CORE, ROWS_ON,
 PART_CORE, PART_X, HALF_RIGHT, HALF_LEFT, SUM_RIGHT, SUM_LEFT) = range(KINDS)


def dot(a, b):
    return jnp.dot(a, b, preferred_element_type=jnp.float32)


def fused(ring, cap_ref, chosen_ref, gates_ref, tok_ref, wg_ref, wu_ref, wd_ref, out_ref,
          near, pick, put, live, rows, w_in, w_out, acc, hid, part_out, part_in, own_sum,
          sum_out, sum_in, far_out, half_in, edges, edge_out, edge_in, own_out,
          send_sem, recv_sem, load_sem, mate_in):
    block, width = tok_ref.shape
    listed = chosen_ref.shape[1]
    half = block // 2
    chunks = width // LANES
    z = lax.axis_index("expert")
    f = lax.axis_index("ffn")
    right = {"expert": lax.rem(z + 1, ring)}
    left = {"expert": lax.rem(z + ring - 1, ring)}
    chip, core = f // 2, f % 2
    slot_id = (f, chip * 2 + 1 - core, (1 - chip) * 2 + core, (1 - chip) * 2 + 1 - core)
    mate = {"ffn": slot_id[1]}
    across = {"ffn": slot_id[2]}

    loads = []
    ff = wg_ref.shape[1]
    for s in range(4):
        at = pl.ds(pl.multiple_of(slot_id[s] * width, width), width)
        loads.append([
            pltpu.make_async_copy(wg_ref.at[at, :], w_in.at[s, :, 0:ff], load_sem.at[3 * s]),
            pltpu.make_async_copy(wu_ref.at[at, :], w_in.at[s, :, ff:2 * ff], load_sem.at[3 * s + 1]),
            pltpu.make_async_copy(wd_ref.at[:, at], w_out.at[s], load_sem.at[3 * s + 2]),
        ])
    for group in loads:
        for load in group:
            load.start()

    barrier = pltpu.get_barrier_semaphore()
    for other in (left, right, across):
        pl.semaphore_signal(barrier, inc=1, device_id=other, device_id_type=MESH)

    @pl.when(core == 0)
    def _():
        pl.semaphore_signal(barrier, inc=1, device_id=mate, device_id_type=MESH)

    @pl.when(core == 0)
    def _():
        pl.semaphore_wait(barrier, 3)

    @pl.when(core == 1)
    def _():
        pl.semaphore_wait(barrier, 4)
        pl.semaphore_signal(mate_in, inc=1, device_id=mate, device_id_type=MESH)

    def cols(q):
        return slice(q * LANES, (q + 1) * LANES)

    def copy(kind, q):
        src, dst, to = {
            TO_RIGHT: lambda: (tok_ref.at[:, cols(q)], near.at[q, 0:block], right),
            TO_LEFT: lambda: (tok_ref.at[:, cols(q)], near.at[q, 2 * block:3 * block], left),
            ON_RIGHT: lambda: (near.at[q, 0:half], near.at[q, block:block + half], right),
            ON_LEFT: lambda: (near.at[q, 2 * block + half:3 * block], near.at[q, block + half:2 * block], left),
            ROWS_X: lambda: (rows.at[0, q], rows.at[2, q], across),
            ROWS_CORE: lambda: (rows.at[0, q], rows.at[1, q], mate),
            ROWS_ON: lambda: (rows.at[2, q], rows.at[3, q], mate),
            PART_CORE: lambda: (part_out.at[q], part_in.at[q], mate),
            PART_X: lambda: (sum_out.at[q], sum_in.at[q], across),
            HALF_RIGHT: lambda: (far_out.at[q, 0:half], half_in.at[q, 0:half], right),
            HALF_LEFT: lambda: (far_out.at[q, half:block], half_in.at[q, half:block], left),
            SUM_RIGHT: lambda: (edge_out.at[q, 0], edge_in.at[q, 0], right),
            SUM_LEFT: lambda: (edge_out.at[q, 1], edge_in.at[q, 1], left),
        }[kind]()
        i = kind * chunks + q
        return pltpu.make_async_remote_copy(
            src_ref=src, dst_ref=dst, send_sem=send_sem.at[i], recv_sem=recv_sem.at[i],
            device_id=to, device_id_type=MESH)

    def start(kind, q):
        copy(kind, q).start()

    def got(kind, q):
        copy(kind, q).wait_recv()

    def own(q):
        start(TO_RIGHT, q)
        start(TO_LEFT, q)

    for q in range(min(2, chunks)):
        own(q)

    ids = chosen_ref[...]

    def mark():
        ids_col = jnp.broadcast_to(ids.astype(jnp.float32), (LANES, listed)).T.astype(jnp.int32)
        lane = lax.broadcasted_iota(jnp.int32, (listed, LANES), 1)
        for r in range(4):
            base = lax.rem(z + ring - r, ring) * block
            for h in range(block // LANES):
                hit = ids_col == lane + (base + h * LANES)
                pick[:, r * block + h * LANES:r * block + (h + 1) * LANES] = jnp.where(hit, 1.0, 0.0).astype(jnp.bfloat16)

    def select(q):
        got(ON_RIGHT, q)
        got(ON_LEFT, q)
        chosen_rows = dot(pick[:, 0:block], tok_ref[:, cols(q)]) + dot(pick[:, block:], near[q])
        rows[0, q] = chosen_rows.astype(jnp.bfloat16)
        start(ROWS_X, q)

    for q in range(chunks):
        got(TO_RIGHT, q)
        start(ON_RIGHT, q)
        got(TO_LEFT, q)
        start(ON_LEFT, q)
        if q + 2 < chunks:
            own(q + 2)
        if q == 0:
            mark()
        else:
            select(q - 1)
    select(chunks - 1)

    @pl.when(core == 0)
    def _():
        pl.semaphore_wait(mate_in, 1)

    for q in range(chunks):
        start(ROWS_CORE, q)

    token = lax.broadcasted_iota(jnp.int32, (block, listed), 0)
    for r in range(4):
        base = lax.rem(z + ring - r, ring) * block
        put[r] = jnp.where(ids == token + base, 1.0, 0.0).astype(jnp.bfloat16)
    position = lax.broadcasted_iota(jnp.int32, (1, listed), 1)
    kept = jnp.where(position < cap_ref[0], gates_ref[...], 0.0)
    live[...] = jnp.broadcast_to(kept, (LANES, listed)).T

    for group in loads:
        for load in group:
            load.wait()

    def whole(s):
        return jnp.concatenate([rows[s, q] for q in range(chunks)], axis=1)

    acc[...] = dot(whole(0), w_in[0])
    for q in range(chunks):
        got(ROWS_CORE, q)
    acc[...] += dot(whole(1), w_in[1])

    def add(s, q):
        acc[...] += dot(rows[s, q], w_in[s, q * LANES:(q + 1) * LANES])

    for q in range(chunks):
        got(ROWS_X, q)
        start(ROWS_ON, q)
        add(2, q)
        if q >= 1:
            got(ROWS_ON, q - 1)
            add(3, q - 1)
    got(ROWS_ON, chunks - 1)
    add(3, chunks - 1)

    gate = acc[:, 0:ff]
    hid[...] = (gate / (1.0 + jnp.exp(-gate)) * acc[:, ff:2 * ff]).astype(jnp.bfloat16)

    for q in range(chunks):
        both = jnp.concatenate([w_out[1, :, cols(q)], w_out[3, :, cols(q)]], axis=1)
        part_out[q] = dot(hid[...], both).astype(jnp.bfloat16)
        start(PART_CORE, q)
    for q in range(chunks):
        both = dot(hid[...], jnp.concatenate([w_out[0, :, cols(q)], w_out[2, :, cols(q)]], axis=1))
        got(PART_CORE, q)
        both = both + part_in[q].astype(jnp.float32)
        sum_out[q] = both[:, LANES:].astype(jnp.bfloat16)
        start(PART_X, q)
        own_sum[q] = both[:, :LANES]

    def finish(q):
        got(SUM_RIGHT, q)
        got(SUM_LEFT, q)
        total = own_out[q] + edge_in[q, 0].astype(jnp.float32) + edge_in[q, 1].astype(jnp.float32)
        out_ref[:, cols(q)] = total.astype(jnp.bfloat16)

    def spread(q):
        got(PART_X, q)
        y = own_sum[q] + sum_in[q].astype(jnp.float32)
        weighted = (live[...] * y).astype(jnp.bfloat16)
        far_out[q] = dot(put[2], weighted).astype(jnp.bfloat16)
        start(HALF_RIGHT, q)
        start(HALF_LEFT, q)
        edges[q, 0] = dot(put[3], weighted)
        edges[q, 1] = dot(put[1], weighted)
        own_out[q] = dot(put[0], weighted)

    def merge(q):
        got(HALF_RIGHT, q)
        edge_out[q, 0, 0:half] = (edges[q, 0, 0:half] + half_in[q, 0:half].astype(jnp.float32)).astype(jnp.bfloat16)
        edge_out[q, 0, half:block] = edges[q, 0, half:block].astype(jnp.bfloat16)
        start(SUM_RIGHT, q)
        got(HALF_LEFT, q)
        edge_out[q, 1, half:block] = (edges[q, 1, half:block] + half_in[q, half:block].astype(jnp.float32)).astype(jnp.bfloat16)
        edge_out[q, 1, 0:half] = edges[q, 1, 0:half].astype(jnp.bfloat16)
        start(SUM_LEFT, q)

    for q in range(chunks + 2):
        if q < chunks:
            spread(q)
        if 1 <= q <= chunks:
            merge(q - 1)
        if q >= 2:
            finish(q - 2)

    for kind in range(KINDS):
        for q in range(chunks):
            copy(kind, q).wait_send()


def shards_fused(ring, tokens, chosen, gates, capacity, w_gate, w_up, w_down):
    block, width = tokens.shape
    listed = chosen.shape[1]
    ff = w_gate.shape[2]
    chunks = width // LANES
    bf16, f32 = jnp.bfloat16, jnp.float32
    vmem = pl.BlockSpec(memory_space=pltpu.VMEM)
    far = pl.BlockSpec(memory_space=pl.ANY)
    return pl.pallas_call(
        functools.partial(fused, ring),
        out_shape=jax.ShapeDtypeStruct(tokens.shape, bf16),
        in_specs=[pl.BlockSpec(memory_space=pltpu.SMEM), vmem, vmem, vmem, far, far, far],
        out_specs=vmem,
        scratch_shapes=[
            pltpu.VMEM((chunks, 3 * block, LANES), bf16),
            pltpu.VMEM((listed, 4 * block), bf16),
            pltpu.VMEM((4, block, listed), bf16),
            pltpu.VMEM((listed, LANES), f32),
            pltpu.VMEM((4, chunks, listed, LANES), bf16),
            pltpu.VMEM((4, width, 2 * ff), bf16),
            pltpu.VMEM((4, ff, width), bf16),
            pltpu.VMEM((listed, 2 * ff), f32),
            pltpu.VMEM((listed, ff), bf16),
            pltpu.VMEM((chunks, listed, 2 * LANES), bf16),
            pltpu.VMEM((chunks, listed, 2 * LANES), bf16),
            pltpu.VMEM((chunks, listed, LANES), f32),
            pltpu.VMEM((chunks, listed, LANES), bf16),
            pltpu.VMEM((chunks, listed, LANES), bf16),
            pltpu.VMEM((chunks, block, LANES), bf16),
            pltpu.VMEM((chunks, block, LANES), bf16),
            pltpu.VMEM((chunks, 2, block, LANES), f32),
            pltpu.VMEM((chunks, 2, block, LANES), bf16),
            pltpu.VMEM((chunks, 2, block, LANES), bf16),
            pltpu.VMEM((chunks, block, LANES), f32),
            pltpu.SemaphoreType.DMA((KINDS * chunks,)),
            pltpu.SemaphoreType.DMA((KINDS * chunks,)),
            pltpu.SemaphoreType.DMA((12,)),
            pltpu.SemaphoreType.REGULAR,
        ],
        compiler_params=pltpu.CompilerParams(collective_id=0, has_side_effects=True),
    )(capacity, chosen, gates, tokens, w_gate[0], w_up[0], w_down[0])


def solution(mesh):
    in_specs = (
        P(("cfg", "expert"), "ffn"),
        P(("cfg", "expert"), None),
        P(("cfg", "expert"), None),
        P("cfg"),
        P("expert", None, "ffn"),
        P("expert", None, "ffn"),
        P("expert", "ffn", None),
    )
    out_specs = P(("cfg", "expert"), "ffn")
    ring = mesh.shape["expert"]
    small = ring == 4 and mesh.shape["ffn"] == 4
    body = functools.partial(shards_fused, ring) if small else shards_general
    return jax.shard_map(body, mesh=mesh, in_specs=in_specs, out_specs=out_specs, check_vma=False)
```

```python
import functools

import jax
import jax.numpy as jnp
from jax import lax
from jax.experimental import pallas as pl
from jax.experimental.pallas import tpu as pltpu
from jax.sharding import PartitionSpec as P


def shards_general(tokens, chosen, gates, capacity, w_gate, w_up, w_down):
    experts_n = lax.axis_size("expert")
    tok_dev = tokens.shape[0]
    picked_ids = chosen[0]
    listed = picked_ids.shape[0]
    slot_depth = 2 * listed // experts_n
    positions = jnp.arange(listed, dtype=jnp.int32)
    alive_mask = positions < capacity[0]
    weights = jnp.where(alive_mask, gates[0], jnp.zeros_like(gates[0]))
    source = picked_ids // tok_dev
    offset = picked_ids - source * tok_dev
    member = (source[:, None] == jnp.arange(experts_n, dtype=jnp.int32)[None, :]).astype(jnp.int32)
    before = jnp.cumsum(member, axis=0) - member
    rank_in = jnp.sum(before * member, axis=1)
    slot_of = source * slot_depth + rank_in
    wanted = jnp.where(alive_mask, offset, -1)
    request = jnp.full((experts_n * slot_depth,), -1, jnp.int32).at[slot_of].set(wanted)
    requested = lax.all_to_all(
        request.reshape(experts_n, slot_depth), "expert", split_axis=0, concat_axis=0, tiled=True
    ).reshape(-1)
    usable = requested >= 0
    safe_idx = jnp.maximum(requested, 0)
    gate_cols = w_gate[0]
    up_cols = w_up[0]
    down_rows = w_down[0]
    row_block = jnp.where(
        usable[:, None], jnp.take(tokens, safe_idx, axis=0), jnp.zeros((), jnp.bfloat16)
    )
    slots = lax.all_to_all(
        row_block.reshape(experts_n, slot_depth, -1),
        "expert",
        split_axis=0,
        concat_axis=0,
        tiled=True,
    )
    picked = jnp.take(slots.reshape(experts_n * slot_depth, -1), slot_of, axis=0)
    portion = lax.all_gather(picked, "ffn", axis=1, tiled=True)
    gate_next = jnp.dot(portion, gate_cols, preferred_element_type=jnp.float32)
    up_next = jnp.dot(portion, up_cols, preferred_element_type=jnp.float32)
    hidden = (jax.nn.silu(gate_next) * up_next).astype(jnp.bfloat16)
    partial_value = jnp.dot(hidden, down_rows, preferred_element_type=jnp.float32)
    summed = lax.psum_scatter(
        partial_value.astype(jnp.bfloat16), "ffn", scatter_dimension=1, tiled=True
    ).astype(jnp.float32)
    contribution = (weights[:, None] * summed).astype(jnp.bfloat16)
    returned_slots = (
        jnp.zeros((experts_n * slot_depth, contribution.shape[1]), jnp.bfloat16)
        .at[slot_of]
        .set(contribution)
    )
    returned = lax.all_to_all(
        returned_slots.reshape(experts_n, slot_depth, -1),
        "expert",
        split_axis=0,
        concat_axis=0,
        tiled=True,
    )
    returned = returned.reshape(experts_n * slot_depth, -1)
    placement_map = (requested[None, :] == jnp.arange(tok_dev, dtype=jnp.int32)[:, None]).astype(
        jnp.bfloat16
    )
    mixed = jnp.dot(placement_map, returned, preferred_element_type=jnp.float32)
    return mixed.astype(jnp.bfloat16)


LANES = 128
KINDS = 15
MESH = pl.DeviceIdType.MESH
(TO_RIGHT, TO_LEFT, ON_RIGHT, ON_LEFT, ROWS_X, ROWS_CORE, ROWS_ON,
 PART_CORE, PART_X, HALF_RIGHT, HALF_LEFT, SUM_RIGHT, SUM_LEFT,
 PLAIN_RIGHT, PLAIN_LEFT) = range(KINDS)


def dot(a, b):
    return jnp.dot(a, b, preferred_element_type=jnp.float32)


def fused(ring, cap_ref, chosen_ref, gates_ref, tok_ref, wg_ref, wu_ref, wd_ref, out_ref,
          near, pick, put, live, rows, w_in, w_out, acc, hid, part_out, part_in, own_sum,
          sum_out, sum_in, far_out, half_in, edges, edge_out, edge_in, own_out,
          send_sem, recv_sem, load_sem, mate_in):
    block, width = tok_ref.shape
    listed = chosen_ref.shape[1]
    half = block // 2
    chunks = width // LANES
    z = lax.axis_index("expert")
    f = lax.axis_index("ffn")

    def member(p):
        return p + (p // 2) * (2 * ring - 3 - 2 * p)

    spot = member(z)
    right = {"expert": member(lax.rem(spot + 1, ring))}
    left = {"expert": member(lax.rem(spot + ring - 1, ring))}
    chip, core = f // 2, f % 2
    slot_id = (f, chip * 2 + 1 - core, (1 - chip) * 2 + core, (1 - chip) * 2 + 1 - core)
    mate = {"ffn": slot_id[1]}
    across = {"ffn": slot_id[2]}

    loads = []
    ff = wg_ref.shape[1]
    for s in range(4):
        at = pl.ds(pl.multiple_of(slot_id[s] * width, width), width)
        loads.append([
            pltpu.make_async_copy(wg_ref.at[at, :], w_in.at[s, :, 0:ff], load_sem.at[3 * s]),
            pltpu.make_async_copy(wu_ref.at[at, :], w_in.at[s, :, ff:2 * ff], load_sem.at[3 * s + 1]),
            pltpu.make_async_copy(wd_ref.at[:, at], w_out.at[s], load_sem.at[3 * s + 2]),
        ])
    for group in loads:
        for load in group:
            load.start()

    barrier = pltpu.get_barrier_semaphore()
    for other in (left, right, across):
        pl.semaphore_signal(barrier, inc=1, device_id=other, device_id_type=MESH)

    @pl.when(core == 0)
    def _():
        pl.semaphore_signal(barrier, inc=1, device_id=mate, device_id_type=MESH)

    @pl.when(core == 0)
    def _():
        pl.semaphore_wait(barrier, 3)

    @pl.when(core == 1)
    def _():
        pl.semaphore_wait(barrier, 4)
        pl.semaphore_signal(mate_in, inc=1, device_id=mate, device_id_type=MESH)

    def cols(q):
        return slice(q * LANES, (q + 1) * LANES)

    def copy(kind, q):
        src, dst, to = {
            TO_RIGHT: lambda: (tok_ref.at[:, cols(q)], near.at[q, 0:block], right),
            TO_LEFT: lambda: (tok_ref.at[:, cols(q)], near.at[q, 2 * block:3 * block], left),
            ON_RIGHT: lambda: (near.at[q, 0:half], near.at[q, block:block + half], right),
            ON_LEFT: lambda: (near.at[q, 2 * block + half:3 * block], near.at[q, block + half:2 * block], left),
            ROWS_X: lambda: (rows.at[0, q], rows.at[2, q], across),
            ROWS_CORE: lambda: (rows.at[0, q], rows.at[1, q], mate),
            ROWS_ON: lambda: (rows.at[2, q], rows.at[3, q], mate),
            PART_CORE: lambda: (part_out.at[q], part_in.at[q], mate),
            PART_X: lambda: (sum_out.at[q], sum_in.at[q], across),
            HALF_RIGHT: lambda: (far_out.at[q, 0:half], half_in.at[q, 0:half], right),
            HALF_LEFT: lambda: (far_out.at[q, half:block], half_in.at[q, half:block], left),
            SUM_RIGHT: lambda: (edge_out.at[q, 0, 0:half], edge_in.at[q, 0, 0:half], right),
            SUM_LEFT: lambda: (edge_out.at[q, 1, half:block], edge_in.at[q, 1, half:block], left),
            PLAIN_RIGHT: lambda: (edge_out.at[q, 0, half:block], edge_in.at[q, 0, half:block], right),
            PLAIN_LEFT: lambda: (edge_out.at[q, 1, 0:half], edge_in.at[q, 1, 0:half], left),
        }[kind]()
        i = kind * chunks + q
        return pltpu.make_async_remote_copy(
            src_ref=src, dst_ref=dst, send_sem=send_sem.at[i], recv_sem=recv_sem.at[i],
            device_id=to, device_id_type=MESH)

    def start(kind, q):
        copy(kind, q).start()

    def got(kind, q):
        copy(kind, q).wait_recv()

    def own(q):
        start(TO_RIGHT, q)
        start(TO_LEFT, q)

    for q in range(min(2, chunks)):
        own(q)

    ids = chosen_ref[...]

    def mark():
        ids_col = jnp.broadcast_to(ids.astype(jnp.float32), (LANES, listed)).T.astype(jnp.int32)
        lane = lax.broadcasted_iota(jnp.int32, (listed, LANES), 1)
        for r in range(4):
            base = member(lax.rem(spot + ring - r, ring)) * block
            for h in range(block // LANES):
                hit = ids_col == lane + (base + h * LANES)
                pick[:, r * block + h * LANES:r * block + (h + 1) * LANES] = jnp.where(hit, 1.0, 0.0).astype(jnp.bfloat16)

    def select(q):
        got(ON_RIGHT, q)
        got(ON_LEFT, q)
        chosen_rows = dot(pick[:, 0:block], tok_ref[:, cols(q)]) + dot(pick[:, block:], near[q])
        rows[0, q] = chosen_rows.astype(jnp.bfloat16)
        start(ROWS_X, q)

    for q in range(chunks):
        got(TO_RIGHT, q)
        start(ON_RIGHT, q)
        got(TO_LEFT, q)
        start(ON_LEFT, q)
        if q + 2 < chunks:
            own(q + 2)
        if q == 0:
            mark()
        else:
            select(q - 1)
    select(chunks - 1)

    @pl.when(core == 0)
    def _():
        pl.semaphore_wait(mate_in, 1)

    for q in range(chunks):
        start(ROWS_CORE, q)

    token = lax.broadcasted_iota(jnp.int32, (block, listed), 0)
    for r in range(4):
        base = member(lax.rem(spot + ring - r, ring)) * block
        put[r] = jnp.where(ids == token + base, 1.0, 0.0).astype(jnp.bfloat16)
    position = lax.broadcasted_iota(jnp.int32, (1, listed), 1)
    kept = jnp.where(position < cap_ref[0], gates_ref[...], 0.0)
    live[...] = jnp.broadcast_to(kept, (LANES, listed)).T

    for group in loads:
        for load in group:
            load.wait()

    def whole(s):
        return jnp.concatenate([rows[s, q] for q in range(chunks)], axis=1)

    acc[...] = dot(whole(0), w_in[0])
    for q in range(chunks):
        got(ROWS_CORE, q)
    acc[...] += dot(whole(1), w_in[1])

    def add(s, q):
        acc[...] += dot(rows[s, q], w_in[s, q * LANES:(q + 1) * LANES])

    for q in range(chunks):
        got(ROWS_X, q)
        start(ROWS_ON, q)
        add(2, q)
        if q >= 1:
            got(ROWS_ON, q - 1)
            add(3, q - 1)
    got(ROWS_ON, chunks - 1)
    add(3, chunks - 1)

    gate = acc[:, 0:ff]
    hid[...] = (gate / (1.0 + jnp.exp(-gate)) * acc[:, ff:2 * ff]).astype(jnp.bfloat16)

    for q in range(chunks):
        both = jnp.concatenate([w_out[1, :, cols(q)], w_out[3, :, cols(q)]], axis=1)
        part_out[q] = dot(hid[...], both).astype(jnp.bfloat16)
        start(PART_CORE, q)
    for q in range(chunks):
        both = dot(hid[...], jnp.concatenate([w_out[0, :, cols(q)], w_out[2, :, cols(q)]], axis=1))
        got(PART_CORE, q)
        both = both + part_in[q].astype(jnp.float32)
        sum_out[q] = both[:, LANES:].astype(jnp.bfloat16)
        start(PART_X, q)
        own_sum[q] = both[:, :LANES]

    def finish(q):
        got(SUM_RIGHT, q)
        got(SUM_LEFT, q)
        got(PLAIN_RIGHT, q)
        got(PLAIN_LEFT, q)
        total = own_out[q] + edge_in[q, 0].astype(jnp.float32) + edge_in[q, 1].astype(jnp.float32)
        out_ref[:, cols(q)] = total.astype(jnp.bfloat16)

    def spread(q):
        got(PART_X, q)
        y = own_sum[q] + sum_in[q].astype(jnp.float32)
        weighted = (live[...] * y).astype(jnp.bfloat16)
        far_out[q] = dot(put[2], weighted).astype(jnp.bfloat16)
        start(HALF_RIGHT, q)
        start(HALF_LEFT, q)
        to_right = dot(put[3], weighted)
        to_left = dot(put[1], weighted)
        edge_out[q, 0, half:block] = to_right[half:block].astype(jnp.bfloat16)
        edge_out[q, 1, 0:half] = to_left[0:half].astype(jnp.bfloat16)
        start(PLAIN_RIGHT, q)
        start(PLAIN_LEFT, q)
        edges[q, 0] = to_right[0:half]
        edges[q, 1] = to_left[half:block]
        own_out[q] = dot(put[0], weighted)

    def merge(q):
        got(HALF_RIGHT, q)
        edge_out[q, 0, 0:half] = (edges[q, 0] + half_in[q, 0:half].astype(jnp.float32)).astype(jnp.bfloat16)
        start(SUM_RIGHT, q)
        got(HALF_LEFT, q)
        edge_out[q, 1, half:block] = (edges[q, 1] + half_in[q, half:block].astype(jnp.float32)).astype(jnp.bfloat16)
        start(SUM_LEFT, q)

    for q in range(chunks + 2):
        if q < chunks:
            spread(q)
        if 1 <= q <= chunks:
            merge(q - 1)
        if q >= 2:
            finish(q - 2)

    for kind in range(KINDS):
        for q in range(chunks):
            copy(kind, q).wait_send()


def shards_fused(ring, tokens, chosen, gates, capacity, w_gate, w_up, w_down):
    block, width = tokens.shape
    listed = chosen.shape[1]
    ff = w_gate.shape[2]
    chunks = width // LANES
    bf16, f32 = jnp.bfloat16, jnp.float32
    vmem = pl.BlockSpec(memory_space=pltpu.VMEM)
    far = pl.BlockSpec(memory_space=pl.ANY)
    return pl.pallas_call(
        functools.partial(fused, ring),
        out_shape=jax.ShapeDtypeStruct(tokens.shape, bf16),
        in_specs=[pl.BlockSpec(memory_space=pltpu.SMEM), vmem, vmem, vmem, far, far, far],
        out_specs=vmem,
        scratch_shapes=[
            pltpu.VMEM((chunks, 3 * block, LANES), bf16),
            pltpu.VMEM((listed, 4 * block), bf16),
            pltpu.VMEM((4, block, listed), bf16),
            pltpu.VMEM((listed, LANES), f32),
            pltpu.VMEM((4, chunks, listed, LANES), bf16),
            pltpu.VMEM((4, width, 2 * ff), bf16),
            pltpu.VMEM((4, ff, width), bf16),
            pltpu.VMEM((listed, 2 * ff), f32),
            pltpu.VMEM((listed, ff), bf16),
            pltpu.VMEM((chunks, listed, 2 * LANES), bf16),
            pltpu.VMEM((chunks, listed, 2 * LANES), bf16),
            pltpu.VMEM((chunks, listed, LANES), f32),
            pltpu.VMEM((chunks, listed, LANES), bf16),
            pltpu.VMEM((chunks, listed, LANES), bf16),
            pltpu.VMEM((chunks, block, LANES), bf16),
            pltpu.VMEM((chunks, block, LANES), bf16),
            pltpu.VMEM((chunks, 2, block // 2, LANES), f32),
            pltpu.VMEM((chunks, 2, block, LANES), bf16),
            pltpu.VMEM((chunks, 2, block, LANES), bf16),
            pltpu.VMEM((chunks, block, LANES), f32),
            pltpu.SemaphoreType.DMA((KINDS * chunks,)),
            pltpu.SemaphoreType.DMA((KINDS * chunks,)),
            pltpu.SemaphoreType.DMA((12,)),
            pltpu.SemaphoreType.REGULAR,
        ],
        compiler_params=pltpu.CompilerParams(collective_id=0, has_side_effects=True),
    )(capacity, chosen, gates, tokens, w_gate[0], w_up[0], w_down[0])


def solution(mesh):
    in_specs = (
        P(("cfg", "expert"), "ffn"),
        P(("cfg", "expert"), None),
        P(("cfg", "expert"), None),
        P("cfg"),
        P("expert", None, "ffn"),
        P("expert", None, "ffn"),
        P("expert", "ffn", None),
    )
    out_specs = P(("cfg", "expert"), "ffn")
    ring = mesh.shape["expert"]
    small = ring == 4 and mesh.shape["ffn"] == 4
    body = functools.partial(shards_fused, ring) if small else shards_general
    return jax.shard_map(body, mesh=mesh, in_specs=in_specs, out_specs=out_specs, check_vma=False)
```
